32 devices in a mesh: section: 4 (over y, x), dp: 8 (over z, core).
Axes of the slice: x: 2, y: 2, z: 4, core: 2. Of those that a mesh axis runs over, the one named last changes fastest.
Arguments:
- hidden_in: bfloat16 [2, 4, 4, 128, 4096], P(None, 'section', None, 'dp'), may hold values from -6 to 6
- out_grad: bfloat16 [4, 128, 4096], P(None, 'dp'), may hold values from -6 to 6
- gate_probs: float32 [2, 4, 4, 128, 2], P(None, 'section', None, 'dp'), may hold values from 0.1 to 1
- expert_ids: int32 [2, 4, 4, 128, 2], P(None, 'section', None, 'dp'), may hold values from 0 to 7, all different within a row
- task_ids: int32 [4, 8], P(None, 'dp'), may hold values from 0 to 1
- task_embed: float32 [2, 256], replicated, may hold values from -5 to 5
- slot_embed: float32 [2, 4, 8, 256], P(None, 'section'), may hold values from -5 to 5
- gen_down: bfloat16 [256, 65536], P(None, 'dp'), may hold values from -0.0078125 to 0.0078125
- gen_up: bfloat16 [256, 65536], P(None, 'dp'), may hold values from -0.09375 to 0.09375
Outputs:
- d_hidden: bfloat16 [4, 4, 128, 4096], P('section', None, 'dp')
- d_gen_down: float32 [256, 65536], P(None, 'dp')
- d_gen_up: float32 [256, 65536], P(None, 'dp')
- d_task_embed: float32 [2, 256], replicated
- d_slot_embed: float32 [2, 4, 8, 256], P(None, 'section')
The draws below stay inside these ranges and needn't reach their ends.
Inputs may be any that keep to these rules, and one draw needn't show every extreme that they name: `expert_ids`: the two experts of a token differ.
All inputs are finite; a program needn't handle non-finite values.
Results may differ from the reference program's by a relative error of at most 0.025.
Values may be sent and summed in bfloat16 or wider, within the bound.
A program may use at most 128 MiB of HBM per device.

```python
import math
import jax
import jax.numpy as jnp
from jax import lax

D = 4096
EXPERTS = 8
RANK = 16
COND = 256
TASKS = 2
BLOCKS = 2
TOK_DEV = 16
MICRO = 4
TOKENS = 128
N_SECTION = 4
N_DP = 8


def touch_ends(drawn, stream_key, least, top_value):
    longest = drawn.shape.index(max(drawn.shape))
    spots = []
    for shift in (0, 1):
        where = [jax.random.randint(jax.random.fold_in(stream_key, axis), (), 0, length) for axis, length in enumerate(drawn.shape)]
        where[longest] = (where[longest] + shift) % drawn.shape[longest]
        spots.append(tuple(where))
    return drawn.at[spots[0]].set(least).at[spots[1]].set(top_value)


def block_levels(own_key, shape, cuts, low, largest):
    loudness = 1.0
    for dim, shards_of in cuts:
        steps = jax.random.uniform(jax.random.fold_in(jax.random.fold_in(own_key, 6), dim), (shards_of,), jnp.float32, low / len(cuts), largest / len(cuts))
        loudness = loudness * jnp.repeat(jnp.exp(steps), shape[dim] // shards_of).reshape((-1,) + (1,) * (len(shape) - 1 - dim))
    return loudness


def different_ones(own_key, rows, count, top, lift):
    sequence = jax.random.permutation(jax.random.fold_in(own_key, 1), count)
    boost = sequence
    for power in range(3):
        boost = boost * boost // count
    boost = boost * lift // count
    lots = jax.random.randint(jax.random.fold_in(own_key, 2), (rows, count), 0, 4096) + boost
    holders = jax.random.permutation(jax.random.fold_in(own_key, 3), rows)[jnp.arange(count) % rows]
    lots = jnp.where(jnp.arange(rows)[:, None] == holders[None, :], 1 << 14, lots)
    score = lots * count + jnp.arange(count)
    return lax.top_k(score.astype(jnp.int32), top)[1].astype(jnp.int32)


def noise(rng, shape, width, reach, shards=(), held_as=jnp.bfloat16):
    values = width * jax.random.normal(rng, shape, jnp.float32)
    if shards:
        values = values * block_levels(rng, shape, shards, -0.22, 0.18)
    return jnp.clip(values, -reach, reach).astype(held_as)


def setup_inputs(seed: int = 0) -> dict:
    keys = jax.random.split(jax.random.key(seed), 10)
    return {
        "hidden_in": noise(keys[0], (BLOCKS, N_SECTION, MICRO, TOKENS, D), 1.0, 6.0, ((1, 4), (3, 8))),
        "out_grad": noise(keys[1], (MICRO, TOKENS, D), 1.0, 6.0, ((1, 8),)),
        "gate_probs": jnp.clip(jnp.exp(math.log(1.0) - 2.3025851 * jax.random.uniform(keys[2], (BLOCKS, N_SECTION, MICRO, TOKENS, 2), jnp.float32) ** block_levels(keys[2], (BLOCKS, N_SECTION, MICRO, TOKENS, 2), ((1, 4), (3, 8)), -0.2, 0.2)), 0.1, 1.0),
        "expert_ids": different_ones(keys[3], BLOCKS * N_SECTION * MICRO * TOKENS, EXPERTS, 2, 2048).reshape((BLOCKS, N_SECTION, MICRO, TOKENS, 2)),
        "task_ids": touch_ends(jax.random.randint(keys[4], (MICRO, N_DP), 0, TASKS), jax.random.fold_in(keys[4], 1), 0, TASKS - 1).astype(jnp.int32),
        "task_embed": noise(keys[5], (TASKS, COND), 1.0, 5.0, (), jnp.float32),
        "slot_embed": noise(keys[6], (BLOCKS, N_SECTION, EXPERTS, COND), 1.0, 5.0, ((1, 4),), jnp.float32),
        "gen_down": noise(keys[7], (COND, RANK * D), (COND * D // 2) ** -0.5, 0.0078125, ((1, 8),)),
        "gen_up": noise(keys[8], (COND, RANK * D), (COND * RANK) ** -0.5, 0.09375, ((1, 8),)),
    }


eps = 1e-05

def column_weights(gates, choices_ids, task_hot, experts, rank):
    expert_hot = (choices_ids[:, :, None] == jnp.arange(experts, dtype=jnp.int32)).astype(jnp.float32)
    per_expert = lax.optimization_barrier(jnp.sum(gates[:, :, None] * expert_hot, axis=1))
    table = task_hot[:, :, None] * per_expert[:, None, :]
    return jnp.repeat(table.reshape(table.shape[0], -1), rank, axis=1)

def layer_back(saved, cot_in, adapt_a, adapt_b, columns):
    values = saved.astype(jnp.float32)
    inv_rms = lax.rsqrt(lax.optimization_barrier(jnp.mean(values * values, axis=-1, keepdims=True)) + eps)
    normed_f = values * inv_rms
    normed = normed_f.astype(jnp.bfloat16)
    contract = (((1,), (1,)), ((), ()))
    low = lax.dot_general(normed, adapt_a, contract, preferred_element_type=jnp.float32)
    mixed_low = (columns * low).astype(jnp.bfloat16)
    back_low = lax.dot_general(cot_in, adapt_b, contract, preferred_element_type=jnp.float32)
    grad_low = (columns * back_low).astype(jnp.bfloat16)
    grad_norm = jnp.dot(grad_low, adapt_a, preferred_element_type=jnp.float32)
    grad_in = inv_rms * (grad_norm - normed_f * lax.optimization_barrier(jnp.mean(grad_norm * normed_f, axis=-1, keepdims=True)))
    result = (cot_in.astype(jnp.float32) + grad_in).astype(jnp.bfloat16)
    return (result, normed, mixed_low, grad_low)

def reference(hidden_in, out_grad, gate_probs, expert_ids, task_ids, task_embed, slot_embed, gen_down, gen_up):
    high = lax.Precision.HIGHEST
    combos = TASKS * EXPERTS
    pre_act = task_embed[None, None, :, None, :] + slot_embed[:, :, None, :, :]
    conditions = jax.nn.silu(pre_act).reshape(BLOCKS, N_SECTION, combos, COND)
    gen_a = jnp.einsum('jscw,wf->jscf', conditions, gen_down.astype(jnp.float32), precision=high).astype(jnp.bfloat16)
    gen_b = jnp.einsum('jscw,wf->jscf', conditions, gen_up.astype(jnp.float32), precision=high).astype(jnp.bfloat16)
    adapt_a = gen_a.reshape(BLOCKS, N_SECTION, combos * RANK, D)
    adapt_b = gen_b.reshape(BLOCKS, N_SECTION, combos * RANK, D)
    token_task = jnp.repeat(task_ids, TOK_DEV, axis=1).reshape(-1)
    task_hot = (token_task[:, None] == jnp.arange(TASKS, dtype=jnp.int32)).astype(jnp.float32)
    rows_contract = (((0,), (0,)), ((), ()))
    cot_now = out_grad.reshape(-1, D)
    grads_a = [[None] * N_SECTION for _ in range(BLOCKS)]
    grads_b = [[None] * N_SECTION for _ in range(BLOCKS)]
    hidden_out = [None] * N_SECTION
    for layer in reversed(range(BLOCKS * N_SECTION)):
        block_id, section_id = divmod(layer, N_SECTION)
        columns = column_weights(gate_probs[block_id, section_id].reshape(-1, 2), expert_ids[block_id, section_id].reshape(-1, 2), task_hot, EXPERTS, RANK)
        cot_prev = cot_now
        cot_now, normed, mixed_low, grad_low = layer_back(hidden_in[block_id, section_id].reshape(-1, D), cot_prev, adapt_a[block_id, section_id], adapt_b[block_id, section_id], columns)
        grads_a[block_id][section_id] = lax.dot_general(grad_low, normed, rows_contract, preferred_element_type=jnp.float32)
        grads_b[block_id][section_id] = lax.dot_general(mixed_low, cot_prev, rows_contract, preferred_element_type=jnp.float32)
        if block_id == 0:
            hidden_out[section_id] = cot_now.reshape(MICRO, TOKENS, D)
    grad_scale = 1.0 / (MICRO * TOKENS)
    full_a = jnp.stack([jnp.stack(line) for line in grads_a]).reshape(BLOCKS, N_SECTION, combos, RANK * D) * grad_scale
    full_b = jnp.stack([jnp.stack(line) for line in grads_b]).reshape(BLOCKS, N_SECTION, combos, RANK * D) * grad_scale
    d_gen_down = jnp.einsum('jscw,jscf->wf', conditions, full_a, precision=high)
    d_gen_up = jnp.einsum('jscw,jscf->wf', conditions, full_b, precision=high)
    d_cond = jnp.einsum('jscf,wf->jscw', full_a, gen_down.astype(jnp.float32), precision=high)
    d_cond = d_cond + jnp.einsum('jscf,wf->jscw', full_b, gen_up.astype(jnp.float32), precision=high)
    sigmoid_pre = jax.nn.sigmoid(pre_act)
    d_pre = d_cond.reshape(pre_act.shape) * sigmoid_pre * (1.0 + pre_act * (1.0 - sigmoid_pre))
    d_task = lax.optimization_barrier(jnp.sum(d_pre, axis=(0, 1, 3)))
    d_slot = lax.optimization_barrier(jnp.sum(d_pre, axis=2))
    return (jnp.stack(hidden_out), d_gen_down, d_gen_up, d_task, d_slot)
```

```python
import functools

import jax
import jax.numpy as jnp
from jax import lax
from jax.experimental import pallas as pl
from jax.experimental.pallas import tpu as pltpu
from jax.sharding import PartitionSpec as P

eps = 1e-05
MESH = pl.DeviceIdType.MESH
nt = (((1,), (1,)), ((), ()))
tn = (((0,), (0,)), ((), ()))


def relay(
    sections, blocks, micro, chunk,
    hid, grad, cols, adapt,
    hid_out, xn_out, cot_out, low_out, glow_out,
    landed, made, wide, send_sem, recv_sem,
):
    me = lax.axis_index("section")
    below = lax.rem(me + sections - 1, sections)
    above = lax.rem(me + 1, sections)
    total = blocks * micro
    groups, _, rows, width = adapt.shape
    ranks = groups * rows
    spans = [pl.ds(at, chunk) for at in range(0, width, chunk)]

    barrier = pltpu.get_barrier_semaphore()
    for other in (below, above):
        pl.semaphore_signal(
            barrier, inc=1, device_id={"section": other}, device_id_type=MESH
        )
    pl.semaphore_wait(barrier, 2)

    def copy_of(item, slot):
        return pltpu.make_async_remote_copy(
            src_ref=made.at[item],
            dst_ref=landed.at[slot],
            send_sem=send_sem.at[item],
            recv_sem=recv_sem.at[slot],
            device_id={"section": below},
            device_id_type=MESH,
        )

    def step(item, carry):
        block = blocks - 1 - item // micro
        spot = block * micro + item % micro
        kind_a, kind_b = 2 * block, 2 * block + 1
        x = hid[spot].astype(jnp.float32)
        inv = lax.rsqrt(jnp.mean(x * x, axis=-1, keepdims=True) + eps)
        xn_out[spot] = (x * inv).astype(jnp.bfloat16)
        weights = cols[spot]
        low = jnp.zeros((x.shape[0], ranks), jnp.float32)
        for span in spans:
            low += lax.dot_general(
                xn_out[spot, :, span], adapt[:, kind_a, :, span].reshape(ranks, chunk), nt,
                preferred_element_type=jnp.float32,
            )
        low_out[spot] = (weights * low).astype(jnp.bfloat16)

        first = (me == sections - 1) & (item < micro)

        @pl.when(first)
        def _():
            landed[item] = grad[item % micro]

        @pl.when(jnp.logical_not(first))
        def _():
            copy_of(item, item).wait_recv()

        cot_out[spot] = landed[item]
        back = jnp.zeros((x.shape[0], ranks), jnp.float32)
        for span in spans:
            back += lax.dot_general(
                landed[item, :, span], adapt[:, kind_b, :, span].reshape(ranks, chunk), nt,
                preferred_element_type=jnp.float32,
            )
        glow = (weights * back).astype(jnp.bfloat16)
        glow_out[spot] = glow
        dots = jnp.zeros((x.shape[0], 1), jnp.float32)
        for span in spans:
            part = jnp.dot(
                glow, adapt[:, kind_a, :, span].reshape(ranks, chunk),
                preferred_element_type=jnp.float32,
            )
            wide[:, span] = part
            xf = hid[spot, :, span].astype(jnp.float32) * inv
            dots += jnp.sum(part * xf, axis=-1, keepdims=True)
        dots = dots * (1.0 / width)
        for span in spans:
            xf = hid[spot, :, span].astype(jnp.float32) * inv
            dx = landed[item, :, span].astype(jnp.float32) + inv * (wide[:, span] - xf * dots)
            made[item, :, span] = dx.astype(jnp.bfloat16)

        @pl.when(me > 0)
        def _():
            copy_of(item, item).start()

        @pl.when((me == 0) & (item < total - micro))
        def _():
            copy_of(item, item + micro).start()

        @pl.when(item >= total - micro)
        def _():
            hid_out[item % micro] = made[item]

        return carry

    lax.fori_loop(0, total, step, 0)

    def drain(item, carry):
        @pl.when((me > 0) | (item < total - micro))
        def _():
            copy_of(item, item).wait_send()

        return carry

    lax.fori_loop(0, total, drain, 0)


def on_device(
    hidden_in, out_grad, gate_probs, expert_ids, task_ids, task_embed, slot_embed, gen_down, gen_up
):
    sections, ways = lax.axis_size("section"), lax.axis_size("dp")
    section_id = lax.axis_index("section")
    blocks, _, micro, tok, width = hidden_in.shape
    tasks, cond_width = task_embed.shape
    experts = slot_embed.shape[2]
    combos = tasks * experts
    span = gen_down.shape[1]
    per = max(1, span // width)
    cuts = max(1, width // span)
    piece = span // per
    kinds = 2 * blocks
    total = blocks * micro

    slots = lax.all_gather(slot_embed[:, 0], "section", axis=0)
    pre_all = task_embed[None, None, :, None, :] + slots[:, :, None, :, :]
    sig_all = jax.nn.sigmoid(pre_all)
    cond_all = (pre_all * sig_all).reshape(-1, cond_width).astype(jnp.bfloat16)
    pre_own = task_embed[None, :, None, :] + slot_embed[:, 0][:, None, :, :]
    cond_own = jax.nn.silu(pre_own).reshape(-1, cond_width).astype(jnp.bfloat16)

    def made_from(gen):
        out = jnp.dot(cond_own, gen, preferred_element_type=jnp.float32).astype(jnp.bfloat16)
        out = out.reshape(blocks, combos, per, piece).transpose(0, 2, 1, 3)
        return out.reshape(blocks, per * combos, piece)

    shard = jnp.stack([made_from(gen_down), made_from(gen_up)], axis=1)
    shard = shard.reshape(1, kinds, per * combos, piece)
    adapt = lax.all_gather(shard, "dp", axis=0, tiled=True)
    if cuts > 1:
        adapt = adapt.reshape(ways // cuts, cuts, kinds, combos, piece).transpose(0, 2, 3, 1, 4)
        adapt = adapt.reshape(ways // cuts, kinds, combos, width)
    groups = adapt.shape[0]
    ranks = groups * per * combos

    hot = (expert_ids[:, 0][..., None] == jnp.arange(experts, dtype=jnp.int32)).astype(jnp.float32)
    per_expert = jnp.sum(gate_probs[:, 0][..., None] * hot, axis=3)
    task_hot = (task_ids == jnp.arange(tasks, dtype=jnp.int32)).astype(jnp.float32)
    table = task_hot[None, :, None, :, None] * per_expert[:, :, :, None, :]
    cols = jnp.tile(table.reshape(total, tok, combos), (1, 1, ranks // combos))

    whole = pl.BlockSpec(memory_space=pltpu.VMEM)
    bf = jnp.bfloat16
    hid_out, xn, cot, low, glow = pl.pallas_call(
        functools.partial(relay, sections, blocks, micro, min(width, 1024)),
        out_shape=(
            jax.ShapeDtypeStruct((micro, tok, width), bf),
            jax.ShapeDtypeStruct((total, tok, width), bf),
            jax.ShapeDtypeStruct((total, tok, width), bf),
            jax.ShapeDtypeStruct((total, tok, ranks), bf),
            jax.ShapeDtypeStruct((total, tok, ranks), bf),
        ),
        in_specs=[whole] * 4,
        out_specs=(whole,) * 5,
        scratch_shapes=[
            pltpu.VMEM((total, tok, width), bf),
            pltpu.VMEM((total, tok, width), bf),
            pltpu.VMEM((tok, width), jnp.float32),
            pltpu.SemaphoreType.DMA((total,)),
            pltpu.SemaphoreType.DMA((total,)),
        ],
        compiler_params=pltpu.CompilerParams(
            collective_id=1, has_side_effects=True, vmem_limit_bytes=40 << 20
        ),
        name="relay",
    )(hidden_in.reshape(total, tok, width), out_grad, cols, adapt)

    scale = 1.0 / (micro * tok * ways)

    def grads(left, right):
        out = lax.dot_general(
            left.reshape(-1, ranks), right.reshape(-1, width), tn,
            preferred_element_type=jnp.float32,
        )
        out = (out * scale).astype(bf)
        if cuts > 1:
            out = out.reshape(ways // cuts, combos, cuts, piece).transpose(0, 2, 1, 3)
        return out.reshape(ways, 1, per * combos, piece)

    reduced = []
    for block in range(blocks):
        at = slice(block * micro, (block + 1) * micro)
        pair = jnp.concatenate([grads(glow[at], xn[at]), grads(low[at], cot[at])], axis=1)
        reduced.append(lax.psum_scatter(pair, "dp", scatter_dimension=0, tiled=True))
    own = jnp.concatenate(reduced, axis=0)
    every = lax.all_gather(own, "section", axis=0, tiled=True)
    every = every.reshape(sections * blocks, 2, per, combos, piece)
    every = every.transpose(1, 0, 3, 2, 4).reshape(2, -1, span)
    part = jnp.zeros((), jnp.float32)
    d_gens = []
    for which, gen in ((0, gen_down), (1, gen_up)):
        d_gens.append(
            lax.dot_general(cond_all, every[which], tn, preferred_element_type=jnp.float32)
        )
        part = part + lax.dot_general(every[which], gen, nt, preferred_element_type=jnp.float32)
    d_pre = part.reshape(pre_all.shape) * sig_all * (1.0 + pre_all * (1.0 - sig_all))
    sums = jnp.concatenate(
        [
            jnp.sum(d_pre, axis=2).reshape(-1, cond_width),
            jnp.sum(d_pre, axis=(0, 1, 3)),
        ]
    )
    sums = lax.psum(sums, "dp")
    d_task = sums[-tasks:]
    d_slot = lax.dynamic_slice_in_dim(
        sums, section_id * blocks * experts, blocks * experts
    ).reshape(blocks, 1, experts, cond_width)
    return (hid_out[None], d_gens[0], d_gens[1], d_task, d_slot)


def solution(mesh):
    placed = (
        P(None, "section", None, "dp", None),
        P(None, "dp", None),
        P(None, "section", None, "dp", None),
        P(None, "section", None, "dp", None),
        P(None, "dp"),
        P(),
        P(None, "section", None, None),
        P(None, "dp"),
        P(None, "dp"),
    )
    return jax.shard_map(
        on_device,
        mesh=mesh,
        in_specs=placed,
        out_specs=(
            P("section", None, "dp", None),
            P(None, "dp"),
            P(None, "dp"),
            P(),
            P(None, "section", None, None),
        ),
        check_vma=False,
    )
```

```python
import functools

import jax
import jax.numpy as jnp
from jax import lax
from jax.experimental import pallas as pl
from jax.experimental.pallas import tpu as pltpu
from jax.sharding import PartitionSpec as P

eps = 1e-05
MESH = pl.DeviceIdType.MESH
nt = (((1,), (1,)), ((), ()))
tn = (((0,), (0,)), ((), ()))


def relay(
    sections, blocks, micro, chunk,
    hid, grad, cols, adapt,
    hid_out, xn_out, cot_out, low_out, glow_out,
    landed, made, wide, send_sem, recv_sem,
):
    me = lax.axis_index("section")
    below = lax.rem(me + sections - 1, sections)
    above = lax.rem(me + 1, sections)
    total = blocks * micro
    groups, _, rows, width = adapt.shape
    ranks = groups * rows
    spans = [pl.ds(at, chunk) for at in range(0, width, chunk)]

    barrier = pltpu.get_barrier_semaphore()
    for other in (below, above):
        pl.semaphore_signal(
            barrier, inc=1, device_id={"section": other}, device_id_type=MESH
        )
    pl.semaphore_wait(barrier, 2)

    def copy_of(item, slot):
        return pltpu.make_async_remote_copy(
            src_ref=made.at[item],
            dst_ref=landed.at[slot],
            send_sem=send_sem.at[item],
            recv_sem=recv_sem.at[slot],
            device_id={"section": below},
            device_id_type=MESH,
        )

    def step(item, carry):
        block = blocks - 1 - item // micro
        spot = block * micro + item % micro
        kind_a, kind_b = 2 * block, 2 * block + 1
        x = hid[spot].astype(jnp.float32)
        inv = lax.rsqrt(jnp.mean(x * x, axis=-1, keepdims=True) + eps)
        xn_out[spot] = (x * inv).astype(jnp.bfloat16)
        weights = cols[spot]
        low = jnp.zeros((x.shape[0], ranks), jnp.float32)
        for span in spans:
            low += lax.dot_general(
                xn_out[spot, :, span], adapt[:, kind_a, :, span].reshape(ranks, chunk), nt,
                preferred_element_type=jnp.float32,
            )
        low_out[spot] = (weights * low).astype(jnp.bfloat16)

        first = (me == sections - 1) & (item < micro)

        @pl.when(first)
        def _():
            landed[item] = grad[item % micro]

        @pl.when(jnp.logical_not(first))
        def _():
            copy_of(item, item).wait_recv()

        cot_out[spot] = landed[item]
        back = jnp.zeros((x.shape[0], ranks), jnp.float32)
        for span in spans:
            back += lax.dot_general(
                landed[item, :, span], adapt[:, kind_b, :, span].reshape(ranks, chunk), nt,
                preferred_element_type=jnp.float32,
            )
        glow = (weights * back).astype(jnp.bfloat16)
        glow_out[spot] = glow
        dots = jnp.zeros((x.shape[0], 1), jnp.float32)
        for span in spans:
            part = jnp.dot(
                glow, adapt[:, kind_a, :, span].reshape(ranks, chunk),
                preferred_element_type=jnp.float32,
            )
            wide[:, span] = part
            xf = hid[spot, :, span].astype(jnp.float32) * inv
            dots += jnp.sum(part * xf, axis=-1, keepdims=True)
        dots = dots * (1.0 / width)
        for span in spans:
            xf = hid[spot, :, span].astype(jnp.float32) * inv
            dx = landed[item, :, span].astype(jnp.float32) + inv * (wide[:, span] - xf * dots)
            made[item, :, span] = dx.astype(jnp.bfloat16)

        @pl.when(me > 0)
        def _():
            copy_of(item, item).start()

        @pl.when((me == 0) & (item < total - micro))
        def _():
            copy_of(item, item + micro).start()

        @pl.when(item >= total - micro)
        def _():
            hid_out[item % micro] = made[item]

        return carry

    lax.fori_loop(0, total, step, 0)

    def drain(item, carry):
        @pl.when((me > 0) | (item < total - micro))
        def _():
            copy_of(item, item).wait_send()

        return carry

    lax.fori_loop(0, total, drain, 0)


def on_device(
    hidden_in, out_grad, gate_probs, expert_ids, task_ids, task_embed, slot_embed, gen_down, gen_up
):
    sections, ways = lax.axis_size("section"), lax.axis_size("dp")
    section_id = lax.axis_index("section")
    blocks, _, micro, tok, width = hidden_in.shape
    tasks, cond_width = task_embed.shape
    experts = slot_embed.shape[2]
    combos = tasks * experts
    span = gen_down.shape[1]
    per = max(1, span // width)
    cuts = max(1, width // span)
    piece = span // per
    kinds = 2 * blocks
    total = blocks * micro

    slots = lax.all_gather(slot_embed[:, 0], "section", axis=0)
    pre_all = task_embed[None, None, :, None, :] + slots[:, :, None, :, :]
    sig_all = jax.nn.sigmoid(pre_all)
    cond_all = (pre_all * sig_all).reshape(-1, cond_width).astype(jnp.bfloat16)
    pre_own = task_embed[None, :, None, :] + slot_embed[:, 0][:, None, :, :]
    cond_own = jax.nn.silu(pre_own).reshape(-1, cond_width).astype(jnp.bfloat16)

    def made_from(gen):
        out = jnp.dot(cond_own, gen, preferred_element_type=jnp.float32).astype(jnp.bfloat16)
        out = out.reshape(blocks, combos, per, piece).transpose(0, 2, 1, 3)
        return out.reshape(blocks, per * combos, piece)

    shard = jnp.stack([made_from(gen_down), made_from(gen_up)], axis=1)
    shard = shard.reshape(1, kinds, per * combos, piece)
    adapt = lax.all_gather(shard, "dp", axis=0, tiled=True)
    if cuts > 1:
        adapt = adapt.reshape(ways // cuts, cuts, kinds, combos, piece).transpose(0, 2, 3, 1, 4)
        adapt = adapt.reshape(ways // cuts, kinds, combos, width)
    groups = adapt.shape[0]
    ranks = groups * per * combos

    hot = (expert_ids[:, 0][..., None] == jnp.arange(experts, dtype=jnp.int32)).astype(jnp.float32)
    per_expert = jnp.sum(gate_probs[:, 0][..., None] * hot, axis=3)
    task_hot = (task_ids == jnp.arange(tasks, dtype=jnp.int32)).astype(jnp.float32)
    table = task_hot[None, :, None, :, None] * per_expert[:, :, :, None, :]
    cols = jnp.tile(table.reshape(total, tok, combos), (1, 1, ranks // combos))

    whole = pl.BlockSpec(memory_space=pltpu.VMEM)
    bf = jnp.bfloat16
    hid_out, xn, cot, low, glow = pl.pallas_call(
        functools.partial(relay, sections, blocks, micro, min(width, 1024)),
        out_shape=(
            jax.ShapeDtypeStruct((micro, tok, width), bf),
            jax.ShapeDtypeStruct((total, tok, width), bf),
            jax.ShapeDtypeStruct((total, tok, width), bf),
            jax.ShapeDtypeStruct((total, tok, ranks), bf),
            jax.ShapeDtypeStruct((total, tok, ranks), bf),
        ),
        in_specs=[whole] * 4,
        out_specs=(whole,) * 5,
        scratch_shapes=[
            pltpu.VMEM((total, tok, width), bf),
            pltpu.VMEM((total, tok, width), bf),
            pltpu.VMEM((tok, width), jnp.float32),
            pltpu.SemaphoreType.DMA((total,)),
            pltpu.SemaphoreType.DMA((total,)),
        ],
        compiler_params=pltpu.CompilerParams(
            collective_id=1, has_side_effects=True, vmem_limit_bytes=40 << 20
        ),
        name="relay",
    )(hidden_in.reshape(total, tok, width), out_grad, cols, adapt)

    scale = 1.0 / (micro * tok * ways)

    def grads(left, right):
        out = lax.dot_general(
            left.reshape(-1, ranks), right.reshape(-1, width), tn,
            preferred_element_type=jnp.float32,
        )
        out = (out * scale).astype(bf)
        if cuts > 1:
            out = out.reshape(ways // cuts, combos, cuts, piece).transpose(0, 2, 1, 3)
        return out.reshape(ways, 1, per * combos, piece)

    reduced = []
    for block in range(blocks):
        at = slice(block * micro, (block + 1) * micro)
        pair = jnp.concatenate([grads(glow[at], xn[at]), grads(low[at], cot[at])], axis=1)
        reduced.append(lax.psum_scatter(pair, "dp", scatter_dimension=0, tiled=True))
    own = jnp.concatenate(reduced, axis=0)
    every = lax.all_gather(own, "section", axis=0, tiled=True)
    every = every.reshape(sections * blocks, 2, per, combos, piece)
    every = every.transpose(1, 0, 3, 2, 4).reshape(2, -1, span)
    part = jnp.zeros((), jnp.float32)
    d_gens = []
    for which, gen in ((0, gen_down), (1, gen_up)):
        d_gens.append(
            lax.dot_general(cond_all, every[which], tn, preferred_element_type=jnp.float32)
        )
        part = part + lax.dot_general(every[which], gen, nt, preferred_element_type=jnp.float32)
    d_pre = part.reshape(pre_all.shape) * sig_all * (1.0 + pre_all * (1.0 - sig_all))
    sums = jnp.concatenate(
        [
            jnp.sum(d_pre, axis=2).reshape(-1, cond_width),
            jnp.sum(d_pre, axis=(0, 1, 3)),
        ]
    )
    sums = jnp.sum(lax.all_gather(sums, "dp", axis=0), axis=0)
    d_task = sums[-tasks:]
    d_slot = lax.dynamic_slice_in_dim(
        sums, section_id * blocks * experts, blocks * experts
    ).reshape(blocks, 1, experts, cond_width)
    return (hid_out[None], d_gens[0], d_gens[1], d_task, d_slot)


def solution(mesh):
    placed = (
        P(None, "section", None, "dp", None),
        P(None, "dp", None),
        P(None, "section", None, "dp", None),
        P(None, "section", None, "dp", None),
        P(None, "dp"),
        P(),
        P(None, "section", None, None),
        P(None, "dp"),
        P(None, "dp"),
    )
    return jax.shard_map(
        on_device,
        mesh=mesh,
        in_specs=placed,
        out_specs=(
            P("section", None, "dp", None),
            P(None, "dp"),
            P(None, "dp"),
            P(),
            P(None, "section", None, None),
        ),
        check_vma=False,
    )
```
